32 devices in a mesh: dom: 32 (over z, y, x, core).
Axes of the slice: x: 2, y: 2, z: 4, core: 2. Of those that a mesh axis runs over, the one named last changes fastest.
Arguments:
- traction: float32 [16384, 3, 128], P('dom'), may hold values from -6 to 6
- fluid_coords: float32 [16384, 3, 128], P('dom'), may hold values from 0 to 1
- struct_coords: float32 [3, 32, 4096], P(None, None, 'dom'), may hold values from 0 to 1
- dest: int32 [16384, 1], P('dom'), may hold values from 0 to 31; in each aligned block of 512 rows (0 to 511, 512 to 1023, ...) at most 32 rows name the same one
- target: int32 [16384], P('dom'), may hold values from 0 to 127
- blocks: float32 [3, 96, 96, 4096], P(None, None, None, 'dom'), may hold values from -1 to 7, as said below
- columns: int32 [2, 4096], P(None, 'dom'), may hold values from 0 to 159
- halo_list: int32 [512], P('dom'), may hold values from 0 to 127
- precond: float32 [96, 96, 4096], P(None, None, 'dom'), may hold values from -1 to 1
Outputs:
- load_field: float32 [96, 4096], P(None, 'dom')
- solution: float32 [96, 4096], P(None, 'dom')
- residual: float32 [96, 4096], P(None, 'dom')
The draws below stay inside these ranges and needn't reach their ends.
Inputs may be any that keep to these rules, and one draw needn't show every extreme that they name: `dest`: among the fluid blocks of one partition no partition is named more than 32 times, a bound that some block reaches. Each diagonal block is its positive diagonal plus small full entries; coupling blocks are small full blocks.
All inputs are finite; a program needn't handle non-finite values.
Results may differ from the reference program's by a relative error of at most 0.0003.
Values sent between devices are 32-bit elements; how exact they have to be, the bound alone decides.
A program may use at most 128 MiB of HBM per device.

```python
import math
import jax
import jax.numpy as jnp
import numpy as np
from jax import lax

NODES = 128
CLUSTER = 96
SNODE = 32
FB_DEV = 512
SB_DEV = 128
HB = 16
ITERS = 2
PARTS_SIZE = 32
CAP = 32
FBLK = 16384
NBLK = 4096
HALO_ALL = 512
N_DOM = 32


def draw_blocks(key, part):
    key_jitter, key_scale = jax.random.split(jax.random.fold_in(key, 11))
    random_part = jnp.clip(jax.random.normal(key_jitter, (3, CLUSTER, CLUSTER, NBLK), jnp.float32), -3.0, 3.0)
    random_part = random_part * (0.5 / math.sqrt(3 * CLUSTER))
    scales = jnp.exp(jax.random.uniform(key_scale, (CLUSTER, NBLK), jnp.float32, math.log(2.0), math.log(6.0)))
    identity = jnp.eye(CLUSTER, dtype=jnp.float32)
    diagonal_part = identity[:, :, None] * scales[:, None, :]
    return random_part.at[0].add(diagonal_part)


def draw_precond(key, part):
    key_jitter, key_scale = jax.random.split(jax.random.fold_in(key, 13))
    random_part = jnp.clip(jax.random.normal(key_jitter, (CLUSTER, CLUSTER, NBLK), jnp.float32), -3.0, 3.0)
    random_part = random_part * (0.1 / math.sqrt(CLUSTER))
    scales = jnp.exp(jax.random.uniform(key_scale, (CLUSTER, NBLK), jnp.float32, math.log(0.15), math.log(0.5)))
    identity = jnp.eye(CLUSTER, dtype=jnp.float32)
    return random_part + identity[:, :, None] * scales[:, None, :]


def touch_ends(values, stream_key, low, high):
    place = [jax.random.randint(jax.random.fold_in(stream_key, axis), (), 0, length) for axis, length in enumerate(values.shape)]
    widest = values.shape.index(max(values.shape))
    next_to = place[:widest] + [(place[widest] + 1) % values.shape[widest]] + place[widest + 1:]
    return values.at[tuple(place)].set(low).at[tuple(next_to)].set(high)


def levels(stream_key, extent, cuts, smallest, high):
    loudness, own = 1.0, jax.random.fold_in(stream_key, 6)
    for dim, parts in cuts:
        heights = jnp.exp(jax.random.uniform(jax.random.fold_in(own, dim), (parts,), jnp.float32, smallest / len(cuts), high / len(cuts)))
        loudness = loudness * jnp.repeat(heights, extent[dim] // parts).reshape([-1 if axis == dim else 1 for axis in range(len(extent))])
    return loudness


def deal_out(key, own, number, rows, count, top, most, lean):
    sequence = jax.random.permutation(key, count)
    packed, usual = load_shares(count, rows * top, most, lean, True), load_shares(count, rows * top, most, lean, False)
    places = jnp.arange(count)

    def named(sizes, offset_by):
        used = int((sizes > 0).sum())
        fixed = max(1, used // 4)
        passed = fixed + (places - fixed + offset_by * (used - fixed)) % max(1, count - fixed)
        return jnp.zeros((count,), jnp.int32).at[sequence[jnp.where(places < fixed, places, passed)]].set(jnp.asarray(sizes, jnp.int32))

    sizes = jnp.where(number % 4 == 0, named(packed, number // 4), named(usual, number - number // 4 - 1))
    mixed = jax.random.permutation(jax.random.fold_in(own, 3), count)
    giver, receiver = mixed[0:count // 2 * 2:2], mixed[1:count // 2 * 2:2]
    slack = jnp.minimum(sizes[giver] - 1, most - sizes[receiver]) // 2
    slack = jnp.where((giver == sequence[0]) | (receiver == sequence[0]) | (sizes[receiver] == 0), 0, jnp.maximum(slack, 0))
    passed = jax.random.randint(jax.random.fold_in(own, 4), (count // 2,), 0, 1 << 20) % (slack + 1)
    sizes = sizes.at[giver].add(-passed).at[receiver].add(passed)
    members = jnp.searchsorted(jnp.cumsum(sizes), jnp.arange(rows * top), side="right").astype(jnp.int32)
    listing = members.reshape(top, rows).T
    listing = listing[jax.random.permutation(jax.random.fold_in(own, 1), rows)]
    offset_by = jax.random.randint(jax.random.fold_in(own, 2), (rows, 1), 0, top)
    return jnp.take_along_axis(listing, (jnp.arange(top)[None, :] + offset_by) % top, axis=1)


def load_shares(number_of, total, most, lean, full):
    portions = [(1 << 20) // math.isqrt(rank ** lean) + 1 for rank in range(1, number_of + 1)]
    largest = most if full else min(most, max(-(-total // number_of), total * portions[0] // sum(portions)))
    least = 1 if total - largest >= number_of - 1 else 0
    given, spare = [largest] + [least] * (number_of - 1), total - largest - least * (number_of - 1)
    while spare > 0:
        candidates = [i for i in range(1, number_of) if given[i] < largest] or [i for i in range(1, number_of) if given[i] < most]
        mass, remaining = sum([portions[i] for i in candidates]), spare
        for i in candidates:
            more = min(most - given[i], max(1, remaining * portions[i] // mass), spare)
            given[i] = given[i] + more
            spare = spare - more
    return np.array(given)


def bell_draw(own_key, extent, width, reach, pieces=(), kind=jnp.bfloat16):
    gain = levels(own_key, extent, pieces, -0.22, 0.18) if pieces else 1.0
    values = jax.random.normal(own_key, extent, jnp.float32) * width * gain
    return jnp.minimum(jnp.maximum(values, -reach), reach).astype(kind)


def setup_inputs(seed: int = 0) -> dict:
    streams_of = jax.random.split(jax.random.key(seed), 10)
    traction = bell_draw(streams_of[0], (FBLK, 3, NODES), 1.0, 6.0, ((0, 32),), jnp.float32)
    fluid_coords = jnp.clip(1.0 * jax.random.uniform(streams_of[1], (FBLK, 3, NODES), jnp.float32) ** levels(streams_of[1], (FBLK, 3, NODES), ((0, 32),), -0.2, 0.2), 0.0, 1.0)
    struct_coords = jnp.clip(1.0 * jax.random.uniform(streams_of[2], (3, SNODE, NBLK), jnp.float32) ** levels(streams_of[2], (3, SNODE, NBLK), ((2, 32),), -0.2, 0.2), 0.0, 1.0)
    dest_keys = jax.random.split(jax.random.fold_in(streams_of[3], 1), FBLK // FB_DEV)
    dest_turns = jax.random.permutation(jax.random.fold_in(streams_of[3], 3), FBLK // FB_DEV)
    dest = jax.vmap(lambda own, number: deal_out(jax.random.fold_in(streams_of[3], 2), own, number, FB_DEV, PARTS_SIZE, 1, CAP, 1))(dest_keys, dest_turns).reshape((FBLK, 1))
    target = touch_ends(jax.random.randint(streams_of[4], (FBLK,), 0, SB_DEV), jax.random.fold_in(streams_of[4], 1), 0, SB_DEV - 1).astype(jnp.int32)
    blocks = draw_blocks(jax.random.fold_in(streams_of[9], 71), 0)
    columns = touch_ends(jax.random.randint(streams_of[6], (2, NBLK), 0, SB_DEV + 2 * HB), jax.random.fold_in(streams_of[6], 1), 0, (SB_DEV + 2 * HB) - 1).astype(jnp.int32)
    halo_list = touch_ends(jax.random.randint(streams_of[7], (HALO_ALL,), 0, SB_DEV), jax.random.fold_in(streams_of[7], 1), 0, SB_DEV - 1).astype(jnp.int32)
    precond = draw_precond(jax.random.fold_in(streams_of[9], 71), 0)
    return dict(traction=traction, fluid_coords=fluid_coords, struct_coords=struct_coords, dest=dest, target=target, blocks=blocks, columns=columns, halo_list=halo_list, precond=precond)


support = 0.9

def wendland_map(fluid_pos, force, struct_pos):
    dist_sq = jnp.zeros((fluid_pos.shape[0], struct_pos.shape[2], fluid_pos.shape[2]), jnp.float32)
    for component in range(3):
        dist_sq = dist_sq + (struct_pos[:, component, :, None] - fluid_pos[:, component, None, :]) ** 2
    radius = jnp.sqrt(dist_sq) / support
    weight = jnp.maximum(1.0 - radius, 0.0) ** 4 * (4.0 * radius + 1.0)
    mapped = jnp.einsum('bjn,bcn->bcj', weight, force, precision=lax.Precision.HIGHEST)
    return mapped.reshape(mapped.shape[0], -1)

def precondition(precond, vector):
    return jnp.einsum('abi,bi->ai', precond, vector, precision=lax.Precision.HIGHEST)

def apply_operator(vector, blocks, columns, halo_list):
    per_part = jnp.transpose(vector.reshape(CLUSTER, N_DOM, SB_DEV), (1, 0, 2))
    listed = halo_list.reshape(N_DOM, HB)
    outgoing = jnp.take_along_axis(per_part, listed[:, None, :], axis=2)
    zero_rim = jnp.zeros_like(outgoing[:1])
    from_left = jnp.concatenate([zero_rim, outgoing[:-1]], axis=0)
    from_right = jnp.concatenate([outgoing[1:], zero_rim], axis=0)
    extended = jnp.concatenate([per_part, from_left, from_right], axis=2)
    result = jnp.einsum('abi,bi->ai', blocks[0], vector, precision=lax.Precision.HIGHEST)
    for neighbor in range(2):
        picks = columns[neighbor].reshape(N_DOM, 1, SB_DEV)
        taken = jnp.take_along_axis(extended, picks, axis=2)
        taken = jnp.transpose(taken, (1, 0, 2)).reshape(CLUSTER, NBLK)
        result = result + jnp.einsum('abi,bi->ai', blocks[neighbor + 1], taken, precision=lax.Precision.HIGHEST)
    return result

def reference(traction, fluid_coords, struct_coords, dest, target, blocks, columns, halo_list, precond):
    global_index = (dest[:, 0] * SB_DEV + target).astype(jnp.int32)

    def per_device(device_index):
        start = (device_index * FB_DEV).astype(jnp.int32)
        positions = lax.dynamic_slice_in_dim(fluid_coords, start, FB_DEV, 0)
        forces = lax.dynamic_slice_in_dim(traction, start, FB_DEV, 0)
        picked = lax.dynamic_slice_in_dim(global_index, start, FB_DEV, 0)
        struct_pos = jnp.transpose(jnp.take(struct_coords, picked, axis=2), (2, 0, 1))
        return wendland_map(positions, forces, struct_pos)
    mapped = lax.map(per_device, jnp.arange(N_DOM, dtype=jnp.int32)).reshape(FBLK, CLUSTER)
    load_field = jax.ops.segment_sum(mapped, global_index, num_segments=NBLK).T
    solution = jnp.zeros_like(load_field)
    residual = load_field
    shadow = load_field
    search = load_field
    alignment = jnp.sum(shadow * residual)
    for step in range(ITERS):
        search_pre = precondition(precond, search)
        image = apply_operator(search_pre, blocks, columns, halo_list)
        step_size = alignment / jnp.sum(shadow * image)
        middle = residual - step_size * image
        middle_pre = precondition(precond, middle)
        middle_image = apply_operator(middle_pre, blocks, columns, halo_list)
        smoothing = jnp.sum(middle_image * middle) / jnp.sum(middle_image * middle_image)
        solution = solution + step_size * search_pre + smoothing * middle_pre
        residual = middle - smoothing * middle_image
        new_alignment = jnp.sum(shadow * residual)
        momentum = new_alignment / alignment * (step_size / smoothing)
        search = residual + momentum * (search - smoothing * image)
        alignment = new_alignment
    return (load_field, solution, residual)
```

```python
import functools

import jax
import jax.numpy as jnp
from jax import lax
from jax.experimental import pallas as pl
from jax.experimental.pallas import tpu as pltpu
from jax.sharding import PartitionSpec as P

support = 0.9


def wendland_map(fluid_pos, force, struct_pos):
    dist_sq = jnp.zeros((fluid_pos.shape[0], struct_pos.shape[2], fluid_pos.shape[2]), jnp.float32)
    for component in range(3):
        dist_sq = (
            dist_sq + (struct_pos[:, component, :, None] - fluid_pos[:, component, None, :]) ** 2
        )
    radius = jnp.sqrt(dist_sq) / support
    weight = jnp.maximum(1.0 - radius, 0.0) ** 4 * (4.0 * radius + 1.0)
    mapped = jnp.einsum("bjn,bcn->bcj", weight, force, precision=lax.Precision.HIGHEST)
    return mapped.reshape(mapped.shape[0], -1)


def split_three(x):
    high = x.astype(jnp.bfloat16)
    rest = x - high.astype(jnp.float32)
    mid = rest.astype(jnp.bfloat16)
    low = (rest - mid.astype(jnp.float32)).astype(jnp.bfloat16)
    return high, mid, low


def pick(pieces, onehot, dims):
    total = None
    for piece in pieces:
        part = lax.dot_general(
            piece, onehot, (dims, ((), ())), preferred_element_type=jnp.float32
        )
        total = part if total is None else total + part
    return total


def krylov_kernel(
    parts,
    load_ref,
    columns_ref,
    halo_ref,
    blocks_hbm,
    precond_hbm,
    solution_ref,
    residual_ref,
    blocks,
    precond,
    operand,
    taken,
    spare,
    halo_out,
    halo_in,
    partial,
    load_sems,
    halo_send,
    halo_recv,
    sum_send,
    sum_recv,
):
    me = lax.axis_index("dom")
    cluster, local = load_ref.shape
    listed = halo_ref.shape[0]
    barrier = pltpu.get_barrier_semaphore()

    loads = [pltpu.make_async_copy(precond_hbm, precond, load_sems.at[0])]
    for which in range(3):
        loads.append(
            pltpu.make_async_copy(
                blocks_hbm.at[which], blocks.at[which], load_sems.at[which + 1]
            )
        )
    for copy in loads:
        copy.start()

    @pl.loop(1, parts)
    def _(k):
        pl.semaphore_signal(
            barrier, 1, device_id=(lax.rem(me + k, parts),), device_id_type=pl.DeviceIdType.MESH
        )

    columns = columns_ref[...]
    rows = lax.broadcasted_iota(jnp.int32, (local, local), 0)
    rim = lax.broadcasted_iota(jnp.int32, (listed, local), 0)

    def hot(cond):
        return jnp.where(cond, 1.0, 0.0).astype(jnp.bfloat16)

    own_hot = [hot(rows == columns[k : k + 1, :]) for k in range(2)]
    left_hot = [hot(rim + local == columns[k : k + 1, :]) for k in range(2)]
    right_hot = [hot(rim + (local + listed) == columns[k : k + 1, :]) for k in range(2)]
    own_hot = jnp.concatenate(own_hot, axis=1)
    left_hot = jnp.concatenate(left_hot, axis=1)
    right_hot = jnp.concatenate(right_hot, axis=1)
    send_hot = hot(lax.broadcasted_iota(jnp.int32, (listed, local), 1) == halo_ref[...])

    group = 8

    def multiply(matrices, vectors, out_ref):
        @pl.loop(0, cluster // group)
        def _(g):
            start = pl.multiple_of(g * group, group)
            for row in range(group):
                total = None
                for matrix, vector in zip(matrices, vectors):
                    term = matrix[pl.ds(start + row, 1)][0] * vector[...]
                    total = term if total is None else total + term
                spare[row : row + 1, :] = jnp.sum(total, axis=0, keepdims=True)
            out_ref[pl.ds(start, group), :] = spare[...]

    def halo_copy(step, side):
        peer = me + 1 if side == 0 else me - 1
        return pltpu.make_async_remote_copy(
            src_ref=halo_out.at[step],
            dst_ref=halo_in.at[step, side],
            send_sem=halo_send.at[step, side],
            recv_sem=halo_recv.at[step, side],
            device_id=(peer,),
            device_id_type=pl.DeviceIdType.MESH,
        )

    def apply(step, vector):
        operand[0] = vector
        if step == 0:
            loads[0].wait()
        multiply([precond], [operand.at[0]], operand.at[1])
        pre = operand[1]
        pieces = split_three(pre)
        outgoing = None
        for piece in pieces:
            part = lax.dot_general(
                send_hot, piece, (((1,), (1,)), ((), ())), preferred_element_type=jnp.float32
            )
            outgoing = part if outgoing is None else outgoing + part
        halo_out[step] = outgoing
        if step == 0:
            pl.semaphore_wait(barrier, parts - 1)

        @pl.when(me < parts - 1)
        def _():
            halo_copy(step, 0).start()

        @pl.when(me > 0)
        def _():
            halo_copy(step, 1).start()

        near = pick(pieces, own_hot, ((1,), (0,)))
        if step == 0:
            for copy in loads[1:]:
                copy.wait()

        @pl.when(me < parts - 1)
        def _():
            halo_copy(step, 0).wait_send()
            halo_copy(step, 1).wait_recv()

        @pl.when(me > 0)
        def _():
            halo_copy(step, 1).wait_send()
            halo_copy(step, 0).wait_recv()

        left = jnp.where(me > 0, halo_in[step, 0], 0.0)
        right = jnp.where(me < parts - 1, halo_in[step, 1], 0.0)
        near = near + pick(split_three(left), left_hot, ((0,), (0,)))
        near = near + pick(split_three(right), right_hot, ((0,), (0,)))
        taken[0] = near[:, :local]
        taken[1] = near[:, local:]
        multiply(
            [blocks.at[0], blocks.at[1], blocks.at[2]],
            [operand.at[1], taken.at[0], taken.at[1]],
            operand.at[2],
        )
        return pre, operand[2]

    lanes = lax.broadcasted_iota(jnp.int32, (1, local), 1)

    def sum_copy(turn, source, target):
        return pltpu.make_async_remote_copy(
            src_ref=partial.at[turn, source],
            dst_ref=partial.at[turn, source],
            send_sem=sum_send.at[turn, target],
            recv_sem=sum_recv.at[turn, source],
            device_id=(target,),
            device_id_type=pl.DeviceIdType.MESH,
        )

    def sums(turn, pairs):
        packed = jnp.zeros((1, local), jnp.float32)
        for index, (x, y) in enumerate(pairs):
            value = jnp.sum(jnp.sum(x * y, axis=0, keepdims=True), axis=1, keepdims=True)
            packed = jnp.where(lanes == index, value, packed)
        partial[turn, me] = packed

        @pl.loop(1, parts)
        def _(k):
            sum_copy(turn, me, lax.rem(me + k, parts)).start()

        @pl.loop(1, parts)
        def _(k):
            other = lax.rem(me + k, parts)
            sum_copy(turn, other, other).wait_recv()
            sum_copy(turn, me, other).wait_send()

        total = jnp.sum(partial[turn], axis=0)
        return [
            jnp.sum(jnp.where(lanes == index, total, 0.0), axis=1, keepdims=True)
            for index in range(len(pairs))
        ]

    v0 = load_ref[...]
    z0, v1 = apply(0, v0)
    z1, v2 = apply(1, v1)
    g00, g01, g02, g11, g12, g22 = sums(
        0, [(v0, v0), (v0, v1), (v0, v2), (v1, v1), (v1, v2), (v2, v2)]
    )
    step_size = g00 / g01
    crossed = g01 - step_size * (g02 + g11) + step_size * step_size * g12
    squared = g11 - 2.0 * step_size * g12 + step_size * step_size * g22
    smoothing = crossed / squared
    solution = step_size * z0 + smoothing * (z0 - step_size * z1)
    residual = (v0 - step_size * v1) - smoothing * (v1 - step_size * v2)
    alignment = (g00 - step_size * g01) - smoothing * (g01 - step_size * g02)
    momentum = (alignment / g00) * (step_size / smoothing)
    search = residual + momentum * (v0 - smoothing * v1)
    p0, image = apply(2, search)
    p1, y = apply(3, image)
    q = image - momentum * (v1 - smoothing * v2)
    pre = p0 - momentum * (z0 - smoothing * z1)
    sr, si, qr, qi, yr, yi, qq, qy, yy = sums(
        1,
        [
            (v0, residual),
            (v0, image),
            (q, residual),
            (q, image),
            (y, residual),
            (y, image),
            (q, q),
            (q, y),
            (y, y),
        ],
    )
    step_size = sr / si
    crossed = qr - step_size * (qi + yr) + step_size * step_size * yi
    squared = qq - 2.0 * step_size * qy + step_size * step_size * yy
    smoothing = crossed / squared
    solution_ref[...] = solution + step_size * p0 + smoothing * (pre - step_size * p1)
    residual_ref[...] = (residual - step_size * image) - smoothing * (q - step_size * y)


def krylov(load_field, columns, halo_list, blocks, precond):
    parts = lax.axis_size("dom")
    cluster, local = load_field.shape
    listed = halo_list.shape[0]
    vmem = pl.BlockSpec(memory_space=pltpu.VMEM)
    hbm = pl.BlockSpec(memory_space=pl.ANY)
    field = jax.ShapeDtypeStruct((cluster, local), jnp.float32)
    f32 = jnp.float32
    return pl.pallas_call(
        functools.partial(krylov_kernel, parts),
        out_shape=(field, field),
        in_specs=[vmem, vmem, vmem, hbm, hbm],
        out_specs=(vmem, vmem),
        scratch_shapes=[
            pltpu.VMEM(blocks.shape, f32),
            pltpu.VMEM(precond.shape, f32),
            pltpu.VMEM((3, cluster, local), f32),
            pltpu.VMEM((2, cluster, local), f32),
            pltpu.VMEM((8, local), f32),
            pltpu.VMEM((4, listed, cluster), f32),
            pltpu.VMEM((4, 2, listed, cluster), f32),
            pltpu.VMEM((2, parts, 1, local), f32),
            pltpu.SemaphoreType.DMA((4,)),
            pltpu.SemaphoreType.DMA((4, 2)),
            pltpu.SemaphoreType.DMA((4, 2)),
            pltpu.SemaphoreType.DMA((2, parts)),
            pltpu.SemaphoreType.DMA((2, parts)),
        ],
        compiler_params=pltpu.CompilerParams(collective_id=0, has_side_effects=True),
        name="krylov",
    )(load_field, columns, halo_list.reshape(-1, 1), blocks, precond)


def on_device(
    traction, fluid_coords, struct_coords, dest, target, blocks, columns, halo_list, precond
):
    partitions = lax.axis_size("dom")
    fluid_count = dest.shape[0]
    cluster = blocks.shape[1]
    local_blocks = blocks.shape[3]
    capacity = max(2, 2 * fluid_count // partitions)
    owner_part = dest[:, 0]
    owner_hits = (owner_part[:, None] == jnp.arange(partitions, dtype=jnp.int32)[None, :]).astype(
        jnp.int32
    )
    before = jnp.sum((jnp.cumsum(owner_hits, axis=0) - owner_hits) * owner_hits, axis=1)
    slot_index = owner_part * capacity + before
    slot_target = jnp.zeros((partitions * capacity,), jnp.int32).at[slot_index].set(target)
    slot_target = slot_target.reshape(partitions, capacity)
    labels = lax.all_to_all(slot_target, "dom", split_axis=0, concat_axis=0, tiled=True)
    onehot = (
        labels.reshape(-1)[:, None] == jnp.arange(local_blocks, dtype=jnp.int32)[None, :]
    ).astype(jnp.float32)
    asked = jnp.dot(
        onehot,
        struct_coords.reshape(-1, local_blocks).T,
        precision=lax.Precision.HIGHEST,
        preferred_element_type=jnp.float32,
    )
    answers = lax.all_to_all(
        asked.reshape(partitions, capacity, cluster),
        "dom",
        split_axis=0,
        concat_axis=0,
        tiled=True,
    )
    answers = answers.reshape(-1, cluster)
    struct_pos = answers.at[slot_index].get(mode="promise_in_bounds")
    struct_pos = struct_pos.reshape(fluid_count, 3, cluster // 3)
    mapped = wendland_map(fluid_coords, traction, struct_pos)
    outgoing = jnp.zeros((partitions * capacity, cluster), jnp.float32).at[slot_index].set(mapped)
    outgoing = outgoing.reshape(partitions, capacity, cluster)
    arrived = lax.all_to_all(outgoing, "dom", split_axis=0, concat_axis=0, tiled=True)
    load_field = jnp.dot(
        arrived.reshape(-1, cluster).T,
        onehot,
        precision=lax.Precision.HIGHEST,
        preferred_element_type=jnp.float32,
    )
    found, rest = krylov(load_field, columns, halo_list, blocks, precond)
    return (load_field, found, rest)


def solution(mesh):
    return jax.shard_map(
        on_device,
        mesh=mesh,
        in_specs=(
            P("dom", None, None),
            P("dom", None, None),
            P(None, None, "dom"),
            P("dom", None),
            P("dom"),
            P(None, None, None, "dom"),
            P(None, "dom"),
            P("dom"),
            P(None, None, "dom"),
        ),
        out_specs=(P(None, "dom"), P(None, "dom"), P(None, "dom")),
        check_vma=False,
    )
```

```python
import functools

import jax
import jax.numpy as jnp
from jax import lax
from jax.experimental import pallas as pl
from jax.experimental.pallas import tpu as pltpu
from jax.sharding import PartitionSpec as P

support = 0.9


def split_three(x):
    high = x.astype(jnp.bfloat16)
    rest = x - high.astype(jnp.float32)
    mid = rest.astype(jnp.bfloat16)
    low = (rest - mid.astype(jnp.float32)).astype(jnp.bfloat16)
    return high, mid, low


def pick(pieces, onehot, dims):
    total = None
    for piece in pieces:
        part = lax.dot_general(
            piece, onehot, (dims, ((), ())), preferred_element_type=jnp.float32
        )
        total = part if total is None else total + part
    return total


def krylov_kernel(
    parts,
    capacity,
    traction_ref,
    fluid_ref,
    struct_ref,
    dest_ref,
    target_ref,
    columns_ref,
    halo_ref,
    blocks_hbm,
    precond_hbm,
    load_ref,
    solution_ref,
    residual_ref,
    blocks,
    precond,
    operand,
    taken,
    spare,
    halo_out,
    halo_in,
    partial,
    labels_out,
    labels_in,
    answers_out,
    answers_in,
    mapped_out,
    mapped_in,
    struct_pos,
    mapped,
    hits,
    exchange_send,
    exchange_recv,
    load_sems,
    halo_send,
    halo_recv,
    sum_send,
    sum_recv,
):
    me = lax.axis_index("dom")
    cluster, local = load_ref.shape
    listed = halo_ref.shape[0]
    count = dest_ref.shape[1]
    nodes = cluster // 3
    barrier = pltpu.get_barrier_semaphore()

    loads = [pltpu.make_async_copy(precond_hbm, precond, load_sems.at[0])]
    for which in range(3):
        loads.append(
            pltpu.make_async_copy(
                blocks_hbm.at[which], blocks.at[which], load_sems.at[which + 1]
            )
        )
    for copy in loads:
        copy.start()

    @pl.loop(1, parts)
    def _(k):
        pl.semaphore_signal(
            barrier, 1, device_id=(lax.rem(me + k, parts),), device_id_type=pl.DeviceIdType.MESH
        )

    columns = columns_ref[...]
    rows = lax.broadcasted_iota(jnp.int32, (local, local), 0)
    rim = lax.broadcasted_iota(jnp.int32, (listed, local), 0)

    def hot(cond):
        return jnp.where(cond, 1.0, 0.0).astype(jnp.bfloat16)

    own_hot = [hot(rows == columns[k : k + 1, :]) for k in range(2)]
    left_hot = [hot(rim + local == columns[k : k + 1, :]) for k in range(2)]
    right_hot = [hot(rim + (local + listed) == columns[k : k + 1, :]) for k in range(2)]
    own_hot = jnp.concatenate(own_hot, axis=1)
    left_hot = jnp.concatenate(left_hot, axis=1)
    right_hot = jnp.concatenate(right_hot, axis=1)
    send_hot = hot(lax.broadcasted_iota(jnp.int32, (listed, local), 1) == halo_ref[...])

    group = 8

    def exchange(turn, source, landing):
        def copy(outgoing, arriving, target, origin):
            return pltpu.make_async_remote_copy(
                src_ref=source.at[outgoing],
                dst_ref=landing.at[arriving],
                send_sem=exchange_send.at[turn, target],
                recv_sem=exchange_recv.at[turn, origin],
                device_id=(target,),
                device_id_type=pl.DeviceIdType.MESH,
            )

        @pl.loop(1, parts)
        def _(k):
            peer = lax.rem(me + k, parts)
            copy(peer, me, peer, me).start()

        landing[me] = source[me]

        @pl.loop(1, parts)
        def _(k):
            peer = lax.rem(me + k, parts)
            copy(peer, peer, peer, peer).wait_recv()
            copy(peer, me, peer, me).wait_send()

    dest = dest_ref[...]
    target = target_ref[...]
    named = lax.broadcasted_iota(jnp.int32, (parts, count), 0) == dest
    earlier = hot(
        lax.broadcasted_iota(jnp.int32, (count, count), 0)
        < lax.broadcasted_iota(jnp.int32, (count, count), 1)
    )
    ahead = jnp.dot(hot(named), earlier, preferred_element_type=jnp.float32)
    rank = jnp.sum(jnp.where(named, ahead, 0.0), axis=0, keepdims=True).astype(jnp.int32)
    slot_row = dest * capacity + rank
    marks = jnp.where(named, target.astype(jnp.float32), 0.0).astype(jnp.bfloat16)
    places = lax.broadcasted_iota(jnp.int32, (local, count), 0)
    ranked = hot(lax.rem(places, capacity) == rank)
    asked = lax.dot_general(
        marks, ranked, (((1,), (1,)), ((), ())), preferred_element_type=jnp.float32
    )
    for part in range(parts):
        labels_out[part] = asked[part : part + 1, :]
    pl.semaphore_wait(barrier, parts - 1)
    exchange(0, labels_out, labels_in)

    per_group = local // capacity
    groups = parts // per_group
    struct_pieces = split_three(struct_ref[...])
    lane_owner = lax.broadcasted_iota(jnp.int32, (1, local), 1) // capacity
    for g in range(groups):
        row = labels_in[g * per_group]
        for member in range(1, per_group):
            row = jnp.where(lane_owner == member, labels_in[g * per_group + member], row)
        hit = hot(rows == row.astype(jnp.int32))
        hits[g] = hit
        found = pick(struct_pieces, hit, ((1,), (0,))).T
        for member in range(per_group):
            answers_out[g * per_group + member] = found[
                member * capacity : (member + 1) * capacity, :
            ]
    exchange(1, answers_out, answers_in)

    side = local
    diagonal = lax.broadcasted_iota(jnp.int32, (side, side), 0) == lax.broadcasted_iota(
        jnp.int32, (side, side), 1
    )
    slots = parts * capacity
    answers = split_three(answers_in[...].reshape(slots, cluster))
    for first in range(0, count, side):
        slot_column = jnp.sum(
            jnp.where(diagonal, slot_row[:, first : first + side], 0).astype(jnp.float32),
            axis=1,
            keepdims=True,
        ).astype(jnp.int32)
        chosen = hot(lax.broadcasted_iota(jnp.int32, (side, slots), 1) == slot_column)
        total = None
        for piece in answers:
            term = jnp.dot(chosen, piece, preferred_element_type=jnp.float32)
            total = term if total is None else total + term
        struct_pos[first : first + side, :] = total * (1.0 / support)

    @pl.loop(0, count // group)
    def _(g):
        start = pl.multiple_of(g * group, group)
        here = pl.ds(start, group)
        positions = struct_pos[here, :]
        fluid = [fluid_ref[c, here, :] * (1.0 / support) for c in range(3)]
        force = [traction_ref[c, here, :] for c in range(3)]
        for j in range(nodes):
            squared = None
            for c in range(3):
                offset = positions[:, c * nodes + j : c * nodes + j + 1] - fluid[c]
                squared = offset * offset if squared is None else squared + offset * offset
            radius = squared * lax.rsqrt(jnp.maximum(squared, 1e-30))
            rest = jnp.maximum(1.0 - radius, 0.0)
            rest = rest * rest
            weight = rest * rest * (4.0 * radius + 1.0)
            for c in range(3):
                mapped[here, c * nodes + j : c * nodes + j + 1] = jnp.sum(
                    weight * force[c], axis=1, keepdims=True
                )

    pieces = split_three(mapped[...])
    for g in range(groups):
        wanted = hot(
            lax.broadcasted_iota(jnp.int32, (local, count), 0) + g * local == slot_row
        )
        total = None
        for piece in pieces:
            term = jnp.dot(wanted, piece, preferred_element_type=jnp.float32)
            total = term if total is None else total + term
        for member in range(per_group):
            mapped_out[g * per_group + member] = total[
                member * capacity : (member + 1) * capacity, :
            ]
    exchange(2, mapped_out, mapped_in)
    arrived = mapped_in[...].reshape(slots, cluster)
    load = None
    for g in range(groups):
        for piece in split_three(arrived[g * local : (g + 1) * local, :]):
            term = jnp.dot(hits[g], piece, preferred_element_type=jnp.float32)
            load = term if load is None else load + term
    load_ref[...] = load.T

    def multiply(matrices, vectors, out_ref):
        @pl.loop(0, cluster // group)
        def _(g):
            start = pl.multiple_of(g * group, group)
            for row in range(group):
                total = None
                for matrix, vector in zip(matrices, vectors):
                    term = matrix[pl.ds(start + row, 1)][0] * vector[...]
                    total = term if total is None else total + term
                spare[row : row + 1, :] = jnp.sum(total, axis=0, keepdims=True)
            out_ref[pl.ds(start, group), :] = spare[...]

    def halo_copy(step, side):
        peer = me + 1 if side == 0 else me - 1
        return pltpu.make_async_remote_copy(
            src_ref=halo_out.at[step],
            dst_ref=halo_in.at[step, side],
            send_sem=halo_send.at[step, side],
            recv_sem=halo_recv.at[step, side],
            device_id=(peer,),
            device_id_type=pl.DeviceIdType.MESH,
        )

    def apply(step, vector):
        operand[0] = vector
        if step == 0:
            loads[0].wait()
        multiply([precond], [operand.at[0]], operand.at[1])
        pre = operand[1]
        pieces = split_three(pre)
        outgoing = None
        for piece in pieces:
            part = lax.dot_general(
                send_hot, piece, (((1,), (1,)), ((), ())), preferred_element_type=jnp.float32
            )
            outgoing = part if outgoing is None else outgoing + part
        halo_out[step] = outgoing
        @pl.when(me < parts - 1)
        def _():
            halo_copy(step, 0).start()

        @pl.when(me > 0)
        def _():
            halo_copy(step, 1).start()

        near = pick(pieces, own_hot, ((1,), (0,)))
        if step == 0:
            for copy in loads[1:]:
                copy.wait()

        @pl.when(me < parts - 1)
        def _():
            halo_copy(step, 0).wait_send()
            halo_copy(step, 1).wait_recv()

        @pl.when(me > 0)
        def _():
            halo_copy(step, 1).wait_send()
            halo_copy(step, 0).wait_recv()

        left = jnp.where(me > 0, halo_in[step, 0], 0.0)
        right = jnp.where(me < parts - 1, halo_in[step, 1], 0.0)
        near = near + pick(split_three(left), left_hot, ((0,), (0,)))
        near = near + pick(split_three(right), right_hot, ((0,), (0,)))
        taken[0] = near[:, :local]
        taken[1] = near[:, local:]
        multiply(
            [blocks.at[0], blocks.at[1], blocks.at[2]],
            [operand.at[1], taken.at[0], taken.at[1]],
            operand.at[2],
        )
        return pre, operand[2]

    lanes = lax.broadcasted_iota(jnp.int32, (1, local), 1)

    def sum_copy(turn, source, target):
        return pltpu.make_async_remote_copy(
            src_ref=partial.at[turn, source],
            dst_ref=partial.at[turn, source],
            send_sem=sum_send.at[turn, target],
            recv_sem=sum_recv.at[turn, source],
            device_id=(target,),
            device_id_type=pl.DeviceIdType.MESH,
        )

    def sums(turn, pairs):
        packed = jnp.zeros((1, local), jnp.float32)
        for index, (x, y) in enumerate(pairs):
            value = jnp.sum(jnp.sum(x * y, axis=0, keepdims=True), axis=1, keepdims=True)
            packed = jnp.where(lanes == index, value, packed)
        partial[turn, me] = packed

        @pl.loop(1, parts)
        def _(k):
            sum_copy(turn, me, lax.rem(me + k, parts)).start()

        @pl.loop(1, parts)
        def _(k):
            other = lax.rem(me + k, parts)
            sum_copy(turn, other, other).wait_recv()
            sum_copy(turn, me, other).wait_send()

        total = jnp.sum(partial[turn], axis=0)
        return [
            jnp.sum(jnp.where(lanes == index, total, 0.0), axis=1, keepdims=True)
            for index in range(len(pairs))
        ]

    v0 = load_ref[...]
    z0, v1 = apply(0, v0)
    z1, v2 = apply(1, v1)
    g00, g01, g02, g11, g12, g22 = sums(
        0, [(v0, v0), (v0, v1), (v0, v2), (v1, v1), (v1, v2), (v2, v2)]
    )
    step_size = g00 / g01
    crossed = g01 - step_size * (g02 + g11) + step_size * step_size * g12
    squared = g11 - 2.0 * step_size * g12 + step_size * step_size * g22
    smoothing = crossed / squared
    solution = step_size * z0 + smoothing * (z0 - step_size * z1)
    residual = (v0 - step_size * v1) - smoothing * (v1 - step_size * v2)
    alignment = (g00 - step_size * g01) - smoothing * (g01 - step_size * g02)
    momentum = (alignment / g00) * (step_size / smoothing)
    search = residual + momentum * (v0 - smoothing * v1)
    p0, image = apply(2, search)
    p1, y = apply(3, image)
    q = image - momentum * (v1 - smoothing * v2)
    pre = p0 - momentum * (z0 - smoothing * z1)
    sr, si, qr, qi, yr, yi, qq, qy, yy = sums(
        1,
        [
            (v0, residual),
            (v0, image),
            (q, residual),
            (q, image),
            (y, residual),
            (y, image),
            (q, q),
            (q, y),
            (y, y),
        ],
    )
    step_size = sr / si
    crossed = qr - step_size * (qi + yr) + step_size * step_size * yi
    squared = qq - 2.0 * step_size * qy + step_size * step_size * yy
    smoothing = crossed / squared
    solution_ref[...] = solution + step_size * p0 + smoothing * (pre - step_size * p1)
    residual_ref[...] = (residual - step_size * image) - smoothing * (q - step_size * y)


def on_device(
    traction, fluid_coords, struct_coords, dest, target, blocks, columns, halo_list, precond
):
    parts = lax.axis_size("dom")
    count = dest.shape[0]
    cluster = blocks.shape[1]
    local = blocks.shape[3]
    listed = halo_list.shape[0]
    capacity = max(2, 2 * count // parts)
    vmem = pl.BlockSpec(memory_space=pltpu.VMEM)
    hbm = pl.BlockSpec(memory_space=pl.ANY)
    f32 = jnp.float32
    field = jax.ShapeDtypeStruct((cluster, local), f32)
    return pl.pallas_call(
        functools.partial(krylov_kernel, parts, capacity),
        out_shape=(field, field, field),
        in_specs=[vmem] * 7 + [hbm] * 2,
        out_specs=(vmem, vmem, vmem),
        scratch_shapes=[
            pltpu.VMEM(blocks.shape, f32),
            pltpu.VMEM(precond.shape, f32),
            pltpu.VMEM((3, cluster, local), f32),
            pltpu.VMEM((2, cluster, local), f32),
            pltpu.VMEM((8, local), f32),
            pltpu.VMEM((4, listed, cluster), f32),
            pltpu.VMEM((4, 2, listed, cluster), f32),
            pltpu.VMEM((2, parts, 1, local), f32),
            pltpu.VMEM((parts, 1, local), f32),
            pltpu.VMEM((parts, 1, local), f32),
            pltpu.VMEM((parts, capacity, cluster), f32),
            pltpu.VMEM((parts, capacity, cluster), f32),
            pltpu.VMEM((parts, capacity, cluster), f32),
            pltpu.VMEM((parts, capacity, cluster), f32),
            pltpu.VMEM((count, cluster), f32),
            pltpu.VMEM((count, cluster), f32),
            pltpu.VMEM((parts * capacity // local, local, local), jnp.bfloat16),
            pltpu.SemaphoreType.DMA((3, parts)),
            pltpu.SemaphoreType.DMA((3, parts)),
            pltpu.SemaphoreType.DMA((4,)),
            pltpu.SemaphoreType.DMA((4, 2)),
            pltpu.SemaphoreType.DMA((4, 2)),
            pltpu.SemaphoreType.DMA((2, parts)),
            pltpu.SemaphoreType.DMA((2, parts)),
        ],
        compiler_params=pltpu.CompilerParams(collective_id=0, has_side_effects=True),
        name="coupling",
    )(
        jnp.transpose(traction, (1, 0, 2)),
        jnp.transpose(fluid_coords, (1, 0, 2)),
        struct_coords.reshape(cluster, local),
        dest.reshape(1, count),
        target.reshape(1, count),
        columns,
        halo_list.reshape(-1, 1),
        blocks,
        precond,
    )


def solution(mesh):
    return jax.shard_map(
        on_device,
        mesh=mesh,
        in_specs=(
            P("dom", None, None),
            P("dom", None, None),
            P(None, None, "dom"),
            P("dom", None),
            P("dom"),
            P(None, None, None, "dom"),
            P(None, "dom"),
            P("dom"),
            P(None, None, "dom"),
        ),
        out_specs=(P(None, "dom"), P(None, "dom"), P(None, "dom")),
        check_vma=False,
    )
```
